32 devices in a mesh: rows: 8 (over y, x, core), cores: 4 (over z).
Axes of the slice: x: 2, y: 2, z: 4, core: 2. Of those that a mesh axis runs over, the one named last changes fastest.
Arguments:
- rhs: float32 [131072, 128], P(('rows', 'cores')), may hold values from -6 to 6
- guess: float32 [131072, 128], P(('rows', 'cores')), may hold values from -4 to 4
- degree: float32 [131072], P(('rows', 'cores')), may hold values from 2 to 6
- weights: bfloat16 [1024, 16, 128, 128], P(('rows', 'cores')), may hold values from -0.1875 to 0.1875
- columns: int32 [1024, 16], P(('rows', 'cores')), may hold values from 0 to 95, as said below
- block_counts: int32 [1024], P(('rows', 'cores')), may hold values from 8 to 16, as said below
- send_lists: int32 [32, 32, 2], P(('rows', 'cores')), may hold values from 0 to 31
- aggregates: int32 [131072], P(('rows', 'cores')), may hold values from 0 to 16383
- coarse_diag: float32 [16384], replicated, may hold values from 4 to 32
Outputs:
- smoothed: float32 [131072, 128], P(('rows', 'cores'))
The draws below stay inside these ranges and needn't reach their ends.
Inputs may be any that keep to these rules, and one draw needn't show every extreme that they name: `block_counts`: every block row has 8 or 16 live slots, and the rows of one device have exactly 320 live slots in all. `columns`: on every device, each table index from 32 up is named by at least one live slot.
All inputs are finite; a program needn't handle non-finite values.
Results may differ from the reference program's by a relative error of at most 0.0022.
Values may be sent and summed in bfloat16 or wider, within the bound.
A program may use at most 128 MiB of HBM per device.

```python
import math
import jax
import jax.numpy as jnp
from jax import lax

NB_DEV = 32
BLOCK = 128
SLOTS = 16
MAXB = 2
RHS = 128
NC = 16384
NBLK = 1024
NV = 131072
DEVICES = 32


def counts_table(key):
    base = jax.random.fold_in(key, 11)
    keys = jax.random.split(base, DEVICES)
    perms = jax.vmap(lambda single: jax.random.permutation(single, NB_DEV))(keys)
    hubby = perms < NB_DEV // 4
    return jnp.where(hubby, SLOTS, SLOTS // 2).astype(jnp.int32)


def draw_block_counts(key, part):
    return counts_table(key).reshape(-1)


def draw_columns(key, part):
    counts = counts_table(key)
    live = (jnp.arange(SLOTS, dtype=jnp.int32)[None, None, :] < counts[:, :, None]).reshape(DEVICES, -1).astype(jnp.int32)
    ranks = jnp.cumsum(live, axis=1) - 1
    remote = DEVICES * MAXB
    livecount = NB_DEV * SLOTS * 5 // 8
    keys = jax.random.split(jax.random.fold_in(key, 23), DEVICES)
    perms = jax.vmap(lambda single: jax.random.permutation(single, livecount))(keys).astype(jnp.int32)
    assigned = jnp.take_along_axis(perms, jnp.clip(ranks, 0, livecount - 1), axis=1)
    filler = jax.random.randint(jax.random.fold_in(key, 31), live.shape, 0, NB_DEV + remote)
    chosen = jnp.where((live == 1) & (assigned < remote), NB_DEV + assigned, filler)
    return chosen.reshape(NB_DEV * DEVICES, SLOTS).astype(jnp.int32)


def draw_aggregates(key, part):
    total = NB_DEV * DEVICES * BLOCK
    per_owner = NC // DEVICES
    device = jnp.arange(total, dtype=jnp.int32) // (NB_DEV * BLOCK)
    inside = jax.random.randint(jax.random.fold_in(key, 41), (total,), 0, per_owner)
    anywhere = jax.random.randint(jax.random.fold_in(key, 47), (total,), 0, NC)
    across = jax.random.randint(jax.random.fold_in(key, 43), (total,), 0, 2) == 0
    own = device * per_owner + inside
    return jnp.where(across, anywhere, own).astype(jnp.int32)


def touch_ends(drawn, rng, low, top_value):
    dims = drawn.shape
    index_at = [jax.random.randint(jax.random.fold_in(rng, axis), (), 0, dims[axis]) for axis in range(len(dims))]
    drawn = drawn.at[tuple(index_at)].set(low)
    longest = dims.index(max(dims))
    index_at[longest] = (index_at[longest] + 1) % dims[longest]
    return drawn.at[tuple(index_at)].set(top_value)


def block_levels(rng, shape, shards, least, high):
    def one(axis_at, shards_of):
        steps = jax.random.uniform(jax.random.fold_in(jax.random.fold_in(rng, 6), axis_at), (shards_of,), jnp.float32, least / len(shards), high / len(shards))
        return jnp.repeat(jnp.exp(steps), shape[axis_at] // shards_of).reshape((-1,) + (1,) * (len(shape) - axis_at - 1))

    loudness = one(*shards[0])
    for cut in shards[1:]:
        loudness = loudness * one(*cut)
    return loudness


def bell_draw(own_key, shape, deviation, bound, shards=(), held_as=jnp.bfloat16):
    level = block_levels(own_key, shape, shards, -0.22, 0.18) if shards else 1.0
    drawn = jax.random.normal(own_key, shape, jnp.float32) * deviation * level
    return jnp.minimum(jnp.maximum(drawn, -bound), bound).astype(held_as)


def setup_inputs(seed: int = 0) -> dict:
    key_of = jax.random.split(jax.random.key(seed), 10)
    return {
        "rhs": bell_draw(key_of[0], (NV, RHS), 1.0, 6.0, ((0, 32),), jnp.float32),
        "guess": bell_draw(key_of[1], (NV, RHS), 0.5, 4.0, ((0, 32),), jnp.float32),
        "degree": jnp.clip(jnp.exp(math.log(6.0) - 1.0986123 * jax.random.uniform(key_of[2], (NV,), jnp.float32) ** block_levels(key_of[2], (NV,), ((0, 32),), -0.2, 0.2)), 2.0, 6.0),
        "weights": bell_draw(key_of[3], (NBLK, SLOTS, BLOCK, BLOCK), (BLOCK * 8) ** -0.5, 0.1875, ((0, 32),)),
        "columns": draw_columns(jax.random.fold_in(key_of[9], 71), 0),
        "block_counts": draw_block_counts(jax.random.fold_in(key_of[9], 71), 0),
        "send_lists": touch_ends(jax.random.randint(key_of[6], (DEVICES, DEVICES, MAXB), 0, NB_DEV), jax.random.fold_in(key_of[6], 1), 0, NB_DEV - 1).astype(jnp.int32),
        "aggregates": draw_aggregates(jax.random.fold_in(key_of[9], 71), 0),
        "coarse_diag": jnp.clip(jnp.exp(jax.random.uniform(key_of[8], (NC,), jnp.float32, math.log(4.0), math.log(32.0))), 4.0, 32.0),
    }


damping = 0.7


def reference(rhs, guess, degree, weights, columns, block_counts, send_lists, aggregates, coarse_diag):
    nblk = weights.shape[0]
    live = (jnp.arange(SLOTS, dtype=jnp.int32)[None, :] < block_counts[:, None]).astype(jnp.bfloat16)
    live_weights = weights * live[:, :, None, None]

    def apply(field):
        blocks = field.astype(jnp.bfloat16).reshape(nblk, BLOCK, RHS)

        def one(device):
            local = lax.dynamic_slice_in_dim(blocks, device * NB_DEV, NB_DEV, 0)
            owners = jnp.arange(DEVICES, dtype=jnp.int32)[:, None] * NB_DEV
            wanted = (owners + send_lists[:, device, :]).reshape(-1).astype(jnp.int32)
            table = jnp.concatenate([local, blocks[wanted]], 0)
            wpart = lax.dynamic_slice_in_dim(live_weights, device * NB_DEV, NB_DEV, 0)
            cpart = lax.dynamic_slice_in_dim(columns, device * NB_DEV, NB_DEV, 0)
            return jnp.einsum('bsij,bsjr->bir', wpart.astype(jnp.float32), table[cpart].astype(jnp.float32))

        offsum = lax.map(one, jnp.arange(DEVICES, dtype=jnp.int32)).reshape(-1, RHS)
        return degree[:, None] * field - offsum

    first = guess + damping * (rhs - apply(guess)) / degree[:, None]
    residue = rhs - apply(first)
    coarse = jax.ops.segment_sum(residue, aggregates, num_segments=NC)
    correction = (coarse / coarse_diag[:, None]).astype(jnp.bfloat16)
    second = first + correction[aggregates].astype(jnp.float32)
    return second + damping * (rhs - apply(second)) / degree[:, None]
```

```python
import functools
import jax
import jax.numpy as jnp
from jax import lax
from jax.experimental import pallas as pl
from jax.experimental.pallas import tpu as pltpu
from jax.sharding import PartitionSpec as P

damping = 0.7
MIB = 1024 * 1024
LIMIT = 64 * 1024 * 1024 - 65536
MESH = pl.DeviceIdType.MESH
VM = pl.BlockSpec(memory_space=pltpu.VMEM)
SM = pl.BlockSpec(memory_space=pltpu.SMEM)
ANY = pl.BlockSpec(memory_space=pl.ANY)
f32, bf16, i32 = jnp.float32, jnp.bfloat16, jnp.int32


def column_of(deg, b):
    row = deg[pl.ds(b, 1), :]
    return jnp.transpose(jnp.broadcast_to(row, (row.shape[1], row.shape[1])))


def row_product(w, tab, cols, b, first, count):
    left = jnp.concatenate([w[b, first + s] for s in range(count)], axis=1)
    right = jnp.concatenate([tab[cols[first + s, b]] for s in range(count)], axis=0)
    return jnp.dot(left, right, preferred_element_type=f32)


def find_full_rows(counts, half, pick, spot):
    nb, extra = spot.shape[0], pick.shape[0]

    def look(b, found):
        rank, rows = found[0], found[1:]
        full = jnp.where(counts[b] > half, 1, 0)
        spot[b] = jnp.where(full == 1, rank, extra)
        rows = [row + jnp.where(rank == e, full * b, 0) for e, row in enumerate(rows)]
        return (rank + full, *rows)

    zero = jnp.zeros((), i32)
    found = lax.fori_loop(0, nb, look, (zero,) * (extra + 1))
    for e in range(extra):
        pick[e] = found[1 + e]


def full_products(w, tab, cols, half, pick, ex):
    for e in range(pick.shape[0]):
        ex[e] = row_product(w, tab, cols, pick[e], half, half)


def vmem(x):
    return pltpu.with_memory_space_constraint(x, pltpu.VMEM)


def each_row(count, step, act):
    @pl.loop(0, count // step)
    def _(i):
        for u in range(step):
            act(i * step + u)


def relax_kernel(nr, nz, guess, rhs_hbm, deg, agg, cols, counts, sends, w_hbm,
                 x1_out, res, ids_out,
                 w, tab1, tab2, pack, aggpack, hagg, dcol, rhs, x1, ex, pick, spot,
                 wsem, bsem, xsem, s1, r1, s2, r2, sa, ra):
    n = nr * nz
    nb, half = w.shape[0], w.shape[1] // 2
    mb = pack.shape[0] // n
    me = lax.axis_index("rows") * nz + lax.axis_index("cores")
    barrier = pltpu.get_barrier_semaphore()

    def where(t):
        return (t // nz, lax.rem(t, nz))

    @pl.loop(1, n)
    def _(k):
        pl.semaphore_signal(barrier, 1, device_id=where(lax.rem(me + k, n)), device_id_type=MESH)

    weights_copy = pltpu.make_async_copy(w_hbm, w, wsem)
    rhs_copy = pltpu.make_async_copy(rhs_hbm, rhs, bsem)
    weights_copy.start()
    rhs_copy.start()

    @pl.loop(0, n)
    def _(t):
        for j in range(mb):
            b = sends[j, t]
            pack[t * mb + j] = guess[b].astype(bf16)
            aggpack[t, pl.ds(j, 1), :] = agg[pl.ds(b, 1), :]

    pl.semaphore_wait(barrier, n - 1)

    def data_copy(k, tab, ss, rr):
        t = lax.rem(me + k, n)
        return pltpu.make_async_remote_copy(
            src_ref=pack.at[pl.ds(t * mb, mb)], dst_ref=tab.at[pl.ds(nb + me * mb, mb)],
            send_sem=ss.at[k], recv_sem=rr.at[k], device_id=where(t), device_id_type=MESH)

    def agg_copy(k):
        t = lax.rem(me + k, n)
        return pltpu.make_async_remote_copy(
            src_ref=aggpack.at[t], dst_ref=hagg.at[me],
            send_sem=sa.at[k], recv_sem=ra.at[k], device_id=where(t), device_id_type=MESH)

    @pl.loop(1, n)
    def _(k):
        data_copy(k, tab1, s1, r1).start()

    @pl.loop(1, n)
    def _(k):
        agg_copy(k).start()

    hagg[me] = aggpack[me]
    for j in range(mb):
        tab1[nb + me * mb + j] = pack[me * mb + j]

    @pl.loop(0, nb)
    def _(b):
        tab1[b] = guess[b].astype(bf16)
        dcol[b] = column_of(deg, b)

    find_full_rows(counts, half, pick, spot)
    ex[pick.shape[0]] = jnp.zeros(ex.shape[1:], f32)
    weights_copy.wait()
    rhs_copy.wait()

    @pl.loop(1, n)
    def _(k):
        data_copy(k, tab1, s1, r1).wait_recv()

    def sweep(b):
        d, g = dcol[b], guess[b]
        off = row_product(w, tab1, cols, b, 0, half) + ex[spot[b]]
        first = g + damping * (rhs[b] - (d * g - off)) / d
        x1[b] = first
        tab2[b] = first.astype(bf16)

    full_products(w, tab1, cols, half, pick, ex)
    each_row(nb, 8, sweep)
    x1_copy = pltpu.make_async_copy(x1, x1_out, xsem)
    x1_copy.start()

    @pl.loop(1, n)
    def _(k):
        data_copy(k, tab1, s1, r1).wait_send()
        agg_copy(k).wait()

    @pl.loop(0, n)
    def _(t):
        for j in range(mb):
            pack[t * mb + j] = x1[sends[j, t]].astype(bf16)

    @pl.loop(1, n)
    def _(k):
        data_copy(k, tab2, s2, r2).start()

    for j in range(mb):
        tab2[nb + me * mb + j] = pack[me * mb + j]
    ids_out[pl.ds(0, nb), :] = agg[...]

    @pl.loop(0, n)
    def _(t):
        ids_out[pl.ds(nb + t * mb, mb), :] = hagg[t]


    @pl.loop(1, n)
    def _(k):
        data_copy(k, tab2, s2, r2).wait_recv()

    def residue(b):
        off = row_product(w, tab2, cols, b, 0, half) + ex[spot[b]]
        res[b] = rhs[b] - (dcol[b] * x1[b] - off)

    full_products(w, tab2, cols, half, pick, ex)
    each_row(nb, 8, residue)

    @pl.loop(1, n)
    def _(k):
        data_copy(k, tab2, s2, r2).wait_send()

    x1_copy.wait()


def restrict_kernel(ways, agg, res, keep, give, *accs):
    for acc in accs:
        acc[...] = jnp.zeros_like(acc)
    span = res.shape[0] // ways
    step = 8

    @pl.loop(0, span // step)
    def _(i):
        for u in range(step):
            places = [agg[q * span + i * step + u] for q in range(ways)]
            sums = [
                accs[q][pl.ds(places[q], 1), :] + res[pl.ds(q * span + i * step + u, 1), :]
                for q in range(ways)
            ]
            for q in range(ways):
                accs[q][pl.ds(places[q], 1), :] = sums[q]

    top = keep.shape[0]
    bit = lax.rem(lax.axis_index("rows"), 2)
    tile = 64

    def total(start):
        rows = pl.ds(pl.multiple_of(start, 16), tile)
        value = accs[0][rows, :]
        for acc in accs[1:]:
            value = value + acc[rows, :]
        return value

    @pl.loop(0, top // tile)
    def _(i):
        rows = pl.ds(i * tile, tile)
        give[rows, :] = total((1 - bit) * top + i * tile).astype(bf16)
        keep[rows, :] = total(bit * top + i * tile)


def cycle_kernel(parts, stages, give, keep, diag, x1_hbm, res, deg, ids_hbm, cols, counts, w_hbm, out,
                 w, first, sbuf, rbuf, corr, fine, tab, ex, base, dcol, dinv, turned, ids, pick, spot,
                 ss, rs, sg, rg, more):
    top = keep.shape[0]
    acc = fine
    nb, half, size = w.shape[0], w.shape[1] // 2, w.shape[2]
    r, z = lax.axis_index("rows"), lax.axis_index("cores")
    barrier = pltpu.get_barrier_semaphore()
    count = len(parts)
    begin = [sum(parts[:p]) for p in range(count)]

    def mine(bit):
        axis, m = bit
        return lax.rem((r if axis == 0 else z) // m, 2)

    def peer(bits, d):
        at, index = [r, z], 0
        for i, bit in enumerate(bits):
            flip = (d >> (len(bits) - 1 - i)) & 1
            b = mine(bit)
            if flip:
                at[bit[0]] = at[bit[0]] + (1 - 2 * b) * bit[1]
                b = 1 - b
            index = index * 2 + b
        return tuple(at), index

    def rows_of(start, tile, i):
        return pl.ds(pl.multiple_of(start + i * tile, 16), tile)

    def tiled(rows, act):
        tile = 64
        while rows % tile:
            tile //= 2

        @pl.loop(0, rows // tile)
        def _(i):
            act(tile, i)

    met = []
    for order in stages:
        for bits in order:
            for d in range(1, 1 << len(bits)):
                key = tuple(sorted(bit for i, bit in enumerate(bits) if (d >> (len(bits) - 1 - i)) & 1))
                if key not in met:
                    met.append(key)
                    pl.semaphore_signal(barrier, 1, device_id=peer(bits, d)[0], device_id_type=MESH)
    pairs = ((ids_hbm, ids), (x1_hbm, base), (w_hbm, w))
    others = [pltpu.make_async_copy(a, b, more.at[k]) for k, (a, b) in enumerate(pairs)]
    others[0].start()
    others[1].start()
    pl.semaphore_wait(barrier, len(met))

    room, slots, at, taken = {}, {}, 0, 0
    for p in range(count):
        left = parts[p]
        for s, bits in enumerate(stages[p]):
            group = 1 << len(bits)
            if s:
                left //= group
            for d in range(1, group):
                slots[p, s, d] = taken
                taken += 1
                if s:
                    room[p, s, d] = (at, left)
                    at += left

    def hop(p, s, d):
        k = slots[p, s, d]
        if s == 0:
            rows = pl.ds(begin[p], parts[p])
            source, target = give.at[rows], first.at[rows]
        else:
            at, left = room[p, s, d]
            rows = pl.ds(at, left)
            source, target = sbuf.at[rows], rbuf.at[rows]
        return pltpu.make_async_remote_copy(
            src_ref=source, dst_ref=target, send_sem=ss.at[k], recv_sem=rs.at[k],
            device_id=peer(stages[p][s], d)[0], device_id_type=MESH)

    for p in range(count):
        hop(p, 0, 1).start()

    find_full_rows(counts, half, pick, spot)
    ex[pick.shape[0]] = jnp.zeros(ex.shape[1:], f32)
    shift = mine(stages[0][0][0]) * top

    def place_of(p):
        place, left = begin[p], parts[p]
        for bits in stages[p][1:]:
            left //= 1 << len(bits)
            place = place + peer(bits, 0)[1] * left
        return place, left

    final = 0
    spots = []
    for p in range(count):
        place, left = place_of(p)
        spots.append(final)

        @pl.loop(0, left // 16)
        def _(i):
            start = shift + place + i * 16
            turned[...] = column_of(diag, start // 128)
            dinv[pl.ds(spots[p] + i * 16, 16), :] = 1.0 / turned[pl.ds(pl.multiple_of(lax.rem(start, 128), 16), 16), :]

        final += left

    def gathered(p, s, start, rows):
        def add(tile, i):
            here = rows_of(start, tile, i)
            if s == 0:
                acc[here, :] = keep[here, :] + first[here, :].astype(f32)
            else:
                total = acc[here, :]
                for d in range(1, 1 << len(stages[p][s])):
                    total = total + rbuf[rows_of(room[p, s, d][0], tile, i), :].astype(f32)
                acc[here, :] = total

        tiled(rows, add)

    regions = list(begin)
    sizes = list(parts)
    levels = max(len(order) for order in stages)
    for s in range(1, levels):
        for p in range(count):
            if s >= len(stages[p]):
                continue
            for d in range(1, 1 << len(stages[p][s - 1])):
                hop(p, s - 1, d).wait_recv()
            gathered(p, s - 1, regions[p], sizes[p])
            bits = stages[p][s]
            left = sizes[p] >> len(bits)
            for d in range(1, 1 << len(bits)):
                start = regions[p] + peer(bits, d)[1] * left
                at = room[p, s, d][0]

                def send(tile, i):
                    sbuf[rows_of(at, tile, i), :] = acc[rows_of(start, tile, i), :].astype(bf16)

                tiled(left, send)
                hop(p, s, d).start()
            regions[p], sizes[p] = regions[p] + peer(bits, 0)[1] * left, left
        if s == 1:
            others[2].start()

            @pl.loop(0, nb)
            def _(b):
                dcol[b] = damping / column_of(deg, b)

            others[1].wait()

            @pl.loop(0, nb)
            def _(b):
                base[b] = base[b] + dcol[b] * res[b]

    def spread(p, s, d, start, left):
        rows = pl.ds(pl.multiple_of(start, 16), left)
        k = slots[p, s, d]
        return pltpu.make_async_remote_copy(
            src_ref=corr.at[rows], dst_ref=corr.at[rows], send_sem=sg.at[k], recv_sem=rg.at[k],
            device_id=peer(stages[p][s], d)[0], device_id_type=MESH)

    def widen(start, rows):
        def act(tile, i):
            fine[rows_of(start, tile, i), :] = corr[rows_of(start, tile, i), :].astype(f32)
        tiled(rows, act)

    sent, waits = [], {}
    for s in reversed(range(levels)):
        for p in range(count):
            last = len(stages[p]) - 1
            if s > last:
                continue
            if s == last:
                for d in range(1, 1 << len(stages[p][s])):
                    hop(p, s, d).wait_recv()
                start, left = regions[p], sizes[p]
                gathered(p, s, start, left)

                def settle(tile, i):
                    corr[rows_of(shift + start, tile, i), :] = (
                        acc[rows_of(start, tile, i), :] * dinv[rows_of(spots[p], tile, i), :]).astype(bf16)

                tiled(left, settle)
            else:
                for copy in waits[p]:
                    copy.wait_recv()
                bits = stages[p][s + 1]
                regions[p] = regions[p] - peer(bits, 0)[1] * sizes[p]
                sizes[p] = sizes[p] << len(bits)
            waits[p] = [
                spread(p, s, d, shift + regions[p], sizes[p]) for d in range(1, 1 << len(stages[p][s]))
            ]
            for copy in waits[p]:
                copy.start()
            sent += waits[p]
            if s == 0:
                widen(shift + begin[p], parts[p])
    others[0].wait()
    for p in range(count):
        for copy in waits[p]:
            copy.wait_recv()
        widen(top - shift + begin[p], parts[p])

    step = 16

    @pl.loop(0, tab.shape[0])
    def _(b):
        for i in range(size // step):
            tab[b, i * step:(i + 1) * step, :] = jnp.concatenate(
                [fine[pl.ds(ids[b * size + i * step + u], 1), :] for u in range(step)], axis=0).astype(bf16)

    others[2].wait()
    full_products(w, tab, cols, half, pick, ex)

    def finish(b):
        off = row_product(w, tab, cols, b, 0, half) + ex[spot[b]]
        out[b] = base[b] + (1.0 - damping) * tab[b].astype(f32) + dcol[b] * off

    each_row(nb, 8, finish)
    for copy in sent:
        copy.wait_send()
    for p, s, d in slots:
        hop(p, s, d).wait_send()


def stage_plan(nr, nz):
    row_bits = [((0, 1 << k),) for k in range(1, nr.bit_length() - 1)]
    z_bits = [(1, 1 << k) for k in range(nz.bit_length() - 1)]
    core = [((0, 1),)]
    swapped = row_bits[::-1]
    apart, together = [(bit,) for bit in z_bits], [tuple(z_bits)]
    a = core + row_bits + together
    b = core + swapped + together
    c = core + apart + row_bits
    d = core + apart + swapped
    return [(c, 2), (d, 2), (a, 6), (b, 6), (c, 2), (d, 2), (a, 6), (b, 6)]


def body(nr, nz, rhs, guess, degree, weights, columns, block_counts, send_lists, aggregates, coarse_diag):
    n = nr * nz
    nb, slots, bs = weights.shape[0], weights.shape[1], weights.shape[2]
    width = rhs.shape[1]
    nc = coarse_diag.shape[0]
    mb = send_lists.shape[2]
    nt = nb + n * mb
    extra = nb // 4
    dma = pltpu.SemaphoreType.DMA
    rhs3, guess3 = rhs.reshape(nb, bs, width), guess.reshape(nb, bs, width)
    deg2, agg2 = degree.reshape(nb, bs), aggregates.reshape(nb, bs)
    field = jax.ShapeDtypeStruct((nb, bs, width), f32)

    x1, res, ids = pl.pallas_call(
        functools.partial(relax_kernel, nr, nz),
        out_shape=(field, pltpu.VMEM((nb, bs, width), f32), jax.ShapeDtypeStruct((nt, bs), i32)),
        in_specs=[VM, ANY, VM, VM, SM, SM, SM, ANY],
        out_specs=(ANY, VM, VM),
        scratch_shapes=[
            pltpu.VMEM((nb, slots, bs, bs), bf16),
            pltpu.VMEM((nt, bs, width), bf16),
            pltpu.VMEM((nt, bs, width), bf16),
            pltpu.VMEM((n * mb, bs, width), bf16),
            pltpu.VMEM((n, mb, bs), i32),
            pltpu.VMEM((n, mb, bs), i32),
            pltpu.VMEM((nb, bs, width), f32),
            pltpu.VMEM((nb, bs, width), f32),
            pltpu.VMEM((nb, bs, width), f32),
            pltpu.VMEM((extra + 1, bs, width), f32),
            pltpu.SMEM((extra,), i32), pltpu.SMEM((nb,), i32),
            dma, dma, dma, dma((n,)), dma((n,)), dma((n,)), dma((n,)), dma((n,)), dma((n,)),
        ],
        compiler_params=pltpu.CompilerParams(
            collective_id=1, has_side_effects=True, vmem_limit_bytes=54 * MIB),
        name="relax",
    )(guess3, rhs3, deg2, agg2, columns.T, block_counts, send_lists[0].T, weights)

    ways = 4
    top = nc // 2
    keep, give = pl.pallas_call(
        functools.partial(restrict_kernel, ways),
        out_shape=(pltpu.VMEM((top, width), f32), pltpu.VMEM((top, width), bf16)),
        in_specs=[SM, VM],
        out_specs=(VM, VM),
        scratch_shapes=[pltpu.VMEM((nc, width), f32)] * ways,
        compiler_params=pltpu.CompilerParams(vmem_limit_bytes=36 * MIB),
        name="restrict",
    )(aggregates, vmem(res.reshape(nb * bs, width)))

    plan = stage_plan(nr, nz)
    stages = [order for order, _ in plan]
    unit = 16 * (n // 2)
    units = top // unit
    whole = sum(weight for _, weight in plan)
    marks = [units * sum(weight for _, weight in plan[:p]) // whole for p in range(len(plan) + 1)]
    parts = [(hi - lo) * unit for lo, hi in zip(marks, marks[1:])]
    stages = [order for order, part in zip(stages, parts) if part]
    parts = [part for part in parts if part]
    hops, moved = 0, 0
    for order, left in zip(stages, parts):
        for s, bits in enumerate(order):
            group = 1 << len(bits)
            hops += group - 1
            if s:
                left //= group
                moved += (group - 1) * left
    out = pl.pallas_call(
        functools.partial(cycle_kernel, parts, stages),
        out_shape=pltpu.VMEM((nb, bs, width), f32),
        in_specs=[VM, VM, VM, ANY, VM, VM, ANY, SM, SM, ANY],
        out_specs=VM,
        scratch_shapes=[
            pltpu.VMEM((nb, slots, bs, bs), bf16),
            pltpu.VMEM((top, width), bf16),
            pltpu.VMEM((moved, width), bf16),
            pltpu.VMEM((moved, width), bf16),
            pltpu.VMEM((nc, width), bf16),
            pltpu.VMEM((nc, width), f32),
            pltpu.VMEM((nt, bs, width), bf16),
            pltpu.VMEM((extra + 1, bs, width), f32),
            pltpu.VMEM((nb, bs, width), f32),
            pltpu.VMEM((nb, bs, width), f32),
            pltpu.VMEM((top // (n // 2), width), f32),
            pltpu.VMEM((bs, width), f32),
            pltpu.SMEM((nt * bs,), i32), pltpu.SMEM((extra,), i32), pltpu.SMEM((nb,), i32),
            dma((hops,)), dma((hops,)), dma((hops,)), dma((hops,)), dma((3,)),
        ],
        compiler_params=pltpu.CompilerParams(
            collective_id=2, has_side_effects=True, vmem_limit_bytes=52 * MIB if nt > 128 else 46 * MIB),
        name="cycle",
    )(vmem(give), vmem(keep), coarse_diag.reshape(nc // bs, bs), x1, vmem(res), deg2, ids.reshape(-1), columns.T, block_counts, weights)
    return out.reshape(nb * bs, width)


def solution(mesh):
    both = ("rows", "cores")
    return jax.shard_map(
        functools.partial(body, mesh.shape["rows"], mesh.shape["cores"]),
        mesh=mesh,
        in_specs=(
            P(both, None), P(both, None), P(both), P(both, None, None, None), P(both, None),
            P(both), P(both, None, None), P(both), P(),
        ),
        out_specs=P(both, None),
        check_vma=False,
    )
```

```python
import functools
import jax
import jax.numpy as jnp
from jax import lax
from jax.experimental import pallas as pl
from jax.experimental.pallas import tpu as pltpu
from jax.sharding import PartitionSpec as P

damping = 0.7
MIB = 1024 * 1024
LIMIT = 64 * 1024 * 1024 - 65536
MESH = pl.DeviceIdType.MESH
VM = pl.BlockSpec(memory_space=pltpu.VMEM)
SM = pl.BlockSpec(memory_space=pltpu.SMEM)
ANY = pl.BlockSpec(memory_space=pl.ANY)
f32, bf16, i32 = jnp.float32, jnp.bfloat16, jnp.int32


def column_of(deg, b):
    row = deg[pl.ds(b, 1), :]
    return jnp.transpose(jnp.broadcast_to(row, (row.shape[1], row.shape[1])))


def row_product(w, tab, cols, b, first, count):
    left = jnp.concatenate([w[b, first + s] for s in range(count)], axis=1)
    right = jnp.concatenate([tab[cols[first + s, b]] for s in range(count)], axis=0)
    return jnp.dot(left, right, preferred_element_type=f32)


def find_full_rows(counts, half, pick, spot):
    nb, extra = spot.shape[0], pick.shape[0]

    def look(b, found):
        rank, rows = found[0], found[1:]
        full = jnp.where(counts[b] > half, 1, 0)
        spot[b] = jnp.where(full == 1, rank, extra)
        rows = [row + jnp.where(rank == e, full * b, 0) for e, row in enumerate(rows)]
        return (rank + full, *rows)

    zero = jnp.zeros((), i32)
    found = lax.fori_loop(0, nb, look, (zero,) * (extra + 1))
    for e in range(extra):
        pick[e] = found[1 + e]


def full_products(w, tab, cols, half, pick, ex):
    for e in range(pick.shape[0]):
        ex[e] = row_product(w, tab, cols, pick[e], half, half)


def vmem(x):
    return pltpu.with_memory_space_constraint(x, pltpu.VMEM)


def each_row(count, step, act):
    @pl.loop(0, count // step)
    def _(i):
        for u in range(step):
            act(i * step + u)


def relax_kernel(nr, nz, guess_hbm, rhs_hbm, deg, agg, cols, counts, sends, w_hbm,
                 x1_out, res, ids_out,
                 w, guess, tab1, tab2, pack, aggpack, hagg, dcol, rhs, x1, ex, pick, spot,
                 wsem, bsem, gsem, xsem, s1, r1, s2, r2, sa, ra):
    n = nr * nz
    nb, half = w.shape[0], w.shape[1] // 2
    mb = pack.shape[0] // n
    me = lax.axis_index("rows") * nz + lax.axis_index("cores")
    barrier = pltpu.get_barrier_semaphore()

    def where(t):
        return (t // nz, lax.rem(t, nz))

    @pl.loop(1, n)
    def _(k):
        pl.semaphore_signal(barrier, 1, device_id=where(lax.rem(me + k, n)), device_id_type=MESH)

    weights_copy = pltpu.make_async_copy(w_hbm, w, wsem)
    rhs_copy = pltpu.make_async_copy(rhs_hbm, rhs, bsem)
    guess_copy = pltpu.make_async_copy(guess_hbm, guess, gsem)
    guess_copy.start()
    guess_copy.wait()
    weights_copy.start()
    rhs_copy.start()

    @pl.loop(0, n)
    def _(t):
        for j in range(mb):
            b = sends[j, t]
            pack[t * mb + j] = guess[b].astype(bf16)
            aggpack[t, pl.ds(j, 1), :] = agg[pl.ds(b, 1), :]

    pl.semaphore_wait(barrier, n - 1)

    def data_copy(k, tab, ss, rr):
        t = lax.rem(me + k, n)
        return pltpu.make_async_remote_copy(
            src_ref=pack.at[pl.ds(t * mb, mb)], dst_ref=tab.at[pl.ds(nb + me * mb, mb)],
            send_sem=ss.at[k], recv_sem=rr.at[k], device_id=where(t), device_id_type=MESH)

    def agg_copy(k):
        t = lax.rem(me + k, n)
        return pltpu.make_async_remote_copy(
            src_ref=aggpack.at[t], dst_ref=hagg.at[me],
            send_sem=sa.at[k], recv_sem=ra.at[k], device_id=where(t), device_id_type=MESH)

    @pl.loop(1, n)
    def _(k):
        data_copy(k, tab1, s1, r1).start()

    @pl.loop(1, n)
    def _(k):
        agg_copy(k).start()

    hagg[me] = aggpack[me]
    for j in range(mb):
        tab1[nb + me * mb + j] = pack[me * mb + j]

    @pl.loop(0, nb)
    def _(b):
        tab1[b] = guess[b].astype(bf16)
        dcol[b] = column_of(deg, b)

    find_full_rows(counts, half, pick, spot)
    ex[pick.shape[0]] = jnp.zeros(ex.shape[1:], f32)
    weights_copy.wait()
    rhs_copy.wait()

    @pl.loop(1, n)
    def _(k):
        data_copy(k, tab1, s1, r1).wait_recv()

    def sweep(b):
        d, g = dcol[b], guess[b]
        off = row_product(w, tab1, cols, b, 0, half) + ex[spot[b]]
        first = g + damping * (rhs[b] - (d * g - off)) / d
        x1[b] = first
        tab2[b] = first.astype(bf16)

    full_products(w, tab1, cols, half, pick, ex)
    each_row(nb, 8, sweep)
    x1_copy = pltpu.make_async_copy(x1, x1_out, xsem)
    x1_copy.start()

    @pl.loop(1, n)
    def _(k):
        data_copy(k, tab1, s1, r1).wait_send()
        agg_copy(k).wait()

    @pl.loop(0, n)
    def _(t):
        for j in range(mb):
            pack[t * mb + j] = x1[sends[j, t]].astype(bf16)

    @pl.loop(1, n)
    def _(k):
        data_copy(k, tab2, s2, r2).start()

    for j in range(mb):
        tab2[nb + me * mb + j] = pack[me * mb + j]
    ids_out[pl.ds(0, nb), :] = agg[...]

    @pl.loop(0, n)
    def _(t):
        ids_out[pl.ds(nb + t * mb, mb), :] = hagg[t]


    @pl.loop(1, n)
    def _(k):
        data_copy(k, tab2, s2, r2).wait_recv()

    def residue(b):
        off = row_product(w, tab2, cols, b, 0, half) + ex[spot[b]]
        res[b] = rhs[b] - (dcol[b] * x1[b] - off)

    full_products(w, tab2, cols, half, pick, ex)
    each_row(nb, 8, residue)

    @pl.loop(1, n)
    def _(k):
        data_copy(k, tab2, s2, r2).wait_send()

    x1_copy.wait()


def split_kernel(nr, nz, guess_hbm, rhs_hbm, deg, agg, cols, counts, sends, w_hbm,
                 x1_out, res, ids_out,
                 w, guess, tab1a, tab1b, tab2a, tab2b, pack1a, pack1b, pack2a, pack2b,
                 aggpack, hagg, dcol, rhs, x1, ex, pick, spot,
                 wsem, bsem, gsem, xsem, s1a, r1a, s1b, r1b, s2a, r2a, s2b, r2b, sa, ra):
    n = nr * nz
    nb, half = w.shape[0], w.shape[1] // 2
    middle = guess.shape[2] // 2
    me = lax.axis_index("rows") * nz + lax.axis_index("cores")
    barrier = pltpu.get_barrier_semaphore()
    left = lax.broadcasted_iota(i32, guess.shape[1:], 1) < middle
    trips = (
        (tab1a, pack1a, s1a, r1a), (tab1b, pack1b, s1b, r1b),
        (tab2a, pack2a, s2a, r2a), (tab2b, pack2b, s2b, r2b),
    )

    def where(t):
        return (t // nz, lax.rem(t, nz))

    def swap(block):
        return pltpu.roll(block, middle, 1)

    @pl.loop(1, n)
    def _(k):
        pl.semaphore_signal(barrier, 1, device_id=where(lax.rem(me + k, n)), device_id_type=MESH)

    weights_copy = pltpu.make_async_copy(w_hbm, w, wsem)
    rhs_copy = pltpu.make_async_copy(rhs_hbm, rhs, bsem)
    guess_copy = pltpu.make_async_copy(guess_hbm, guess, gsem)
    guess_copy.start()

    def packed(field, side, t):
        one, two = field[sends[0, t]], field[sends[1, t]]
        return (jnp.where(left, one, swap(two)) if side == 0 else jnp.where(left, swap(one), two)).astype(bf16)

    def data_copy(trip, k):
        tab, pack, ss, rr = trips[trip]
        t = lax.rem(me + k, n)
        return pltpu.make_async_remote_copy(
            src_ref=pack.at[t], dst_ref=tab.at[nb + me * 2 + trip % 2],
            send_sem=ss.at[k], recv_sem=rr.at[k], device_id=where(t), device_id_type=MESH)

    def send_all(trip):
        @pl.loop(1, n)
        def _(k):
            data_copy(trip, k).start()

    def take_all(trip):
        tab, side = trips[trip][0], trip % 2
        tab[nb + me * 2 + side] = trips[trip][1][me]

        @pl.loop(1, n)
        def _(k):
            data_copy(trip, k).wait_recv()

        @pl.loop(0, n)
        def _(t):
            tab[nb + t * 2 + 1 - side] = swap(tab[nb + t * 2 + side].astype(f32)).astype(bf16)

    def agg_copy(k):
        t = lax.rem(me + k, n)
        return pltpu.make_async_remote_copy(
            src_ref=aggpack.at[t], dst_ref=hagg.at[me],
            send_sem=sa.at[k], recv_sem=ra.at[k], device_id=where(t), device_id_type=MESH)

    guess_copy.wait()

    @pl.loop(0, n)
    def _(t):
        pack1a[t] = packed(guess, 0, t)

    pl.semaphore_wait(barrier, n - 1)
    send_all(0)
    weights_copy.start()
    rhs_copy.start()

    @pl.loop(0, n)
    def _(t):
        pack1b[t] = packed(guess, 1, t)
        for j in range(2):
            aggpack[t, pl.ds(j, 1), :] = agg[pl.ds(sends[j, t], 1), :]

    send_all(1)

    @pl.loop(1, n)
    def _(k):
        agg_copy(k).start()

    hagg[me] = aggpack[me]

    @pl.loop(0, nb)
    def _(b):
        block = guess[b].astype(bf16)
        tab1a[b] = block
        tab1b[b] = block
        dcol[b] = column_of(deg, b)

    find_full_rows(counts, half, pick, spot)
    ex[pick.shape[0]] = jnp.zeros(ex.shape[1:], f32)
    weights_copy.wait()
    rhs_copy.wait()

    def sweep(side):
        tab = trips[side][0]

        def act(b):
            d, g = dcol[b], guess[b]
            off = row_product(w, tab, cols, b, 0, half) + ex[spot[b]]
            fresh = g + damping * (rhs[b] - (d * g - off)) / d
            if side:
                fresh = jnp.where(left, x1[b], fresh)
            x1[b] = fresh
            trips[2 + side][0][b] = fresh.astype(bf16)

        take_all(side)
        full_products(w, tab, cols, half, pick, ex)
        each_row(nb, 8, act)
        pack = trips[2 + side][1]

        @pl.loop(0, n)
        def _(t):
            pack[t] = packed(x1, side, t)

        send_all(2 + side)

    sweep(0)
    sweep(1)
    x1_copy = pltpu.make_async_copy(x1, x1_out, xsem)
    x1_copy.start()

    @pl.loop(1, n)
    def _(k):
        agg_copy(k).wait()

    ids_out[pl.ds(0, nb), :] = agg[...]

    @pl.loop(0, n)
    def _(t):
        ids_out[pl.ds(nb + t * 2, 2), :] = hagg[t]

    def residue(side):
        tab = trips[2 + side][0]

        def act(b):
            off = row_product(w, tab, cols, b, 0, half) + ex[spot[b]]
            fresh = rhs[b] - (dcol[b] * x1[b] - off)
            res[b] = jnp.where(left, res[b], fresh) if side else fresh

        take_all(2 + side)
        full_products(w, tab, cols, half, pick, ex)
        each_row(nb, 8, act)

    residue(0)
    residue(1)
    for trip in range(4):
        @pl.loop(1, n)
        def _(k):
            data_copy(trip, k).wait_send()

    x1_copy.wait()


def restrict_kernel(ways, agg, res, keep, give, *accs):
    for acc in accs:
        acc[...] = jnp.zeros_like(acc)
    span = res.shape[0] // ways
    step = 8

    @pl.loop(0, span // step)
    def _(i):
        for u in range(step):
            places = [agg[q * span + i * step + u] for q in range(ways)]
            sums = [
                accs[q][pl.ds(places[q], 1), :] + res[pl.ds(q * span + i * step + u, 1), :]
                for q in range(ways)
            ]
            for q in range(ways):
                accs[q][pl.ds(places[q], 1), :] = sums[q]

    top = keep.shape[0]
    bit = lax.rem(lax.axis_index("rows"), 2)
    tile = 64

    def total(start):
        rows = pl.ds(pl.multiple_of(start, 16), tile)
        value = accs[0][rows, :]
        for acc in accs[1:]:
            value = value + acc[rows, :]
        return value

    @pl.loop(0, top // tile)
    def _(i):
        rows = pl.ds(i * tile, tile)
        give[rows, :] = total((1 - bit) * top + i * tile).astype(bf16)
        keep[rows, :] = total(bit * top + i * tile)


def cycle_kernel(parts, stages, give, keep, diag, x1_hbm, res, deg, ids_hbm, cols, counts, w_hbm, out,
                 w, first, sbuf, rbuf, corr, fine, tab, ex, base, dcol, dinv, turned, ids, pick, spot,
                 ss, rs, sg, rg, more):
    top = keep.shape[0]
    acc = fine
    nb, half, size = w.shape[0], w.shape[1] // 2, w.shape[2]
    r, z = lax.axis_index("rows"), lax.axis_index("cores")
    barrier = pltpu.get_barrier_semaphore()
    count = len(parts)
    begin = [sum(parts[:p]) for p in range(count)]

    def mine(bit):
        axis, m = bit
        return lax.rem((r if axis == 0 else z) // m, 2)

    def peer(bits, d):
        at, index = [r, z], 0
        for i, bit in enumerate(bits):
            flip = (d >> (len(bits) - 1 - i)) & 1
            b = mine(bit)
            if flip:
                at[bit[0]] = at[bit[0]] + (1 - 2 * b) * bit[1]
                b = 1 - b
            index = index * 2 + b
        return tuple(at), index

    def rows_of(start, tile, i):
        return pl.ds(pl.multiple_of(start + i * tile, 16), tile)

    def tiled(rows, act):
        tile = 64
        while rows % tile:
            tile //= 2

        @pl.loop(0, rows // tile)
        def _(i):
            act(tile, i)

    met = []
    for order in stages:
        for bits in order:
            for d in range(1, 1 << len(bits)):
                key = tuple(sorted(bit for i, bit in enumerate(bits) if (d >> (len(bits) - 1 - i)) & 1))
                if key not in met:
                    met.append(key)
                    pl.semaphore_signal(barrier, 1, device_id=peer(bits, d)[0], device_id_type=MESH)
    pairs = ((ids_hbm, ids), (x1_hbm, base), (w_hbm, w))
    others = [pltpu.make_async_copy(a, b, more.at[k]) for k, (a, b) in enumerate(pairs)]
    others[0].start()
    others[1].start()
    pl.semaphore_wait(barrier, len(met))

    room, slots, at, taken = {}, {}, 0, 0
    for p in range(count):
        left = parts[p]
        for s, bits in enumerate(stages[p]):
            group = 1 << len(bits)
            if s:
                left //= group
            for d in range(1, group):
                slots[p, s, d] = taken
                taken += 1
                if s:
                    room[p, s, d] = (at, left)
                    at += left

    def hop(p, s, d):
        k = slots[p, s, d]
        if s == 0:
            rows = pl.ds(begin[p], parts[p])
            source, target = give.at[rows], first.at[rows]
        else:
            at, left = room[p, s, d]
            rows = pl.ds(at, left)
            source, target = sbuf.at[rows], rbuf.at[rows]
        return pltpu.make_async_remote_copy(
            src_ref=source, dst_ref=target, send_sem=ss.at[k], recv_sem=rs.at[k],
            device_id=peer(stages[p][s], d)[0], device_id_type=MESH)

    for p in range(count):
        hop(p, 0, 1).start()

    find_full_rows(counts, half, pick, spot)
    ex[pick.shape[0]] = jnp.zeros(ex.shape[1:], f32)
    shift = mine(stages[0][0][0]) * top

    def place_of(p):
        place, left = begin[p], parts[p]
        for bits in stages[p][1:]:
            left //= 1 << len(bits)
            place = place + peer(bits, 0)[1] * left
        return place, left

    final = 0
    spots = []
    for p in range(count):
        place, left = place_of(p)
        spots.append(final)

        @pl.loop(0, left // 16)
        def _(i):
            start = shift + place + i * 16
            turned[...] = column_of(diag, start // 128)
            dinv[pl.ds(spots[p] + i * 16, 16), :] = 1.0 / turned[pl.ds(pl.multiple_of(lax.rem(start, 128), 16), 16), :]

        final += left

    def gathered(p, s, start, rows):
        def add(tile, i):
            here = rows_of(start, tile, i)
            if s == 0:
                acc[here, :] = keep[here, :] + first[here, :].astype(f32)
            else:
                total = acc[here, :]
                for d in range(1, 1 << len(stages[p][s])):
                    total = total + rbuf[rows_of(room[p, s, d][0], tile, i), :].astype(f32)
                acc[here, :] = total

        tiled(rows, add)

    regions = list(begin)
    sizes = list(parts)
    levels = max(len(order) for order in stages)
    for s in range(1, levels):
        for p in range(count):
            if s >= len(stages[p]):
                continue
            for d in range(1, 1 << len(stages[p][s - 1])):
                hop(p, s - 1, d).wait_recv()
            gathered(p, s - 1, regions[p], sizes[p])
            bits = stages[p][s]
            left = sizes[p] >> len(bits)
            for d in range(1, 1 << len(bits)):
                start = regions[p] + peer(bits, d)[1] * left
                at = room[p, s, d][0]

                def send(tile, i):
                    sbuf[rows_of(at, tile, i), :] = acc[rows_of(start, tile, i), :].astype(bf16)

                tiled(left, send)
                hop(p, s, d).start()
            regions[p], sizes[p] = regions[p] + peer(bits, 0)[1] * left, left
        if s == 1:
            others[2].start()

            @pl.loop(0, nb)
            def _(b):
                dcol[b] = damping / column_of(deg, b)

            others[1].wait()

            @pl.loop(0, nb)
            def _(b):
                base[b] = base[b] + dcol[b] * res[b]

    def spread(p, s, d, start, left):
        rows = pl.ds(pl.multiple_of(start, 16), left)
        k = slots[p, s, d]
        return pltpu.make_async_remote_copy(
            src_ref=corr.at[rows], dst_ref=corr.at[rows], send_sem=sg.at[k], recv_sem=rg.at[k],
            device_id=peer(stages[p][s], d)[0], device_id_type=MESH)

    def widen(start, rows):
        def act(tile, i):
            fine[rows_of(start, tile, i), :] = corr[rows_of(start, tile, i), :].astype(f32)
        tiled(rows, act)

    sent, waits = [], {}
    for s in reversed(range(levels)):
        for p in range(count):
            last = len(stages[p]) - 1
            if s > last:
                continue
            if s == last:
                for d in range(1, 1 << len(stages[p][s])):
                    hop(p, s, d).wait_recv()
                start, left = regions[p], sizes[p]
                gathered(p, s, start, left)

                def settle(tile, i):
                    corr[rows_of(shift + start, tile, i), :] = (
                        acc[rows_of(start, tile, i), :] * dinv[rows_of(spots[p], tile, i), :]).astype(bf16)

                tiled(left, settle)
            else:
                for copy in waits[p]:
                    copy.wait_recv()
                bits = stages[p][s + 1]
                regions[p] = regions[p] - peer(bits, 0)[1] * sizes[p]
                sizes[p] = sizes[p] << len(bits)
            waits[p] = [
                spread(p, s, d, shift + regions[p], sizes[p]) for d in range(1, 1 << len(stages[p][s]))
            ]
            for copy in waits[p]:
                copy.start()
            sent += waits[p]
            if s == 0:
                widen(shift + begin[p], parts[p])
    others[0].wait()
    for p in range(count):
        for copy in waits[p]:
            copy.wait_recv()
        widen(top - shift + begin[p], parts[p])

    step = 16

    @pl.loop(0, tab.shape[0])
    def _(b):
        for i in range(size // step):
            tab[b, i * step:(i + 1) * step, :] = jnp.concatenate(
                [fine[pl.ds(ids[b * size + i * step + u], 1), :] for u in range(step)], axis=0).astype(bf16)

    others[2].wait()
    full_products(w, tab, cols, half, pick, ex)

    def finish(b):
        off = row_product(w, tab, cols, b, 0, half) + ex[spot[b]]
        out[b] = base[b] + (1.0 - damping) * tab[b].astype(f32) + dcol[b] * off

    each_row(nb, 8, finish)
    for copy in sent:
        copy.wait_send()
    for p, s, d in slots:
        hop(p, s, d).wait_send()


def stage_plan(nr, nz):
    row_bits = [((0, 1 << k),) for k in range(1, nr.bit_length() - 1)]
    z_bits = [(1, 1 << k) for k in range(nz.bit_length() - 1)]
    core = [((0, 1),)]
    swapped = row_bits[::-1]
    apart, together = [(bit,) for bit in z_bits], [tuple(z_bits)]
    a = core + row_bits + together
    b = core + swapped + together
    c = core + apart + row_bits
    d = core + apart + swapped
    return 4 * [(a, 3), (b, 3), (c, 1), (d, 1)]


def body(nr, nz, rhs, guess, degree, weights, columns, block_counts, send_lists, aggregates, coarse_diag):
    n = nr * nz
    nb, slots, bs = weights.shape[0], weights.shape[1], weights.shape[2]
    width = rhs.shape[1]
    nc = coarse_diag.shape[0]
    mb = send_lists.shape[2]
    nt = nb + n * mb
    extra = nb // 4
    dma = pltpu.SemaphoreType.DMA
    rhs3, guess3 = rhs.reshape(nb, bs, width), guess.reshape(nb, bs, width)
    deg2, agg2 = degree.reshape(nb, bs), aggregates.reshape(nb, bs)
    field = jax.ShapeDtypeStruct((nb, bs, width), f32)

    table, message = pltpu.VMEM((nt, bs, width), bf16), pltpu.VMEM((n, bs, width), bf16)
    split = mb == 2 and nt <= 4 * nb
    if split:
        kernel, tables, trips = split_kernel, [table] * 4 + [message] * 4, 4
    else:
        kernel, tables, trips = relax_kernel, [table] * 2 + [pltpu.VMEM((n * mb, bs, width), bf16)], 2
    x1, res, ids = pl.pallas_call(
        functools.partial(kernel, nr, nz),
        out_shape=(field, pltpu.VMEM((nb, bs, width), f32), jax.ShapeDtypeStruct((nt, bs), i32)),
        in_specs=[ANY, ANY, VM, VM, SM, SM, SM, ANY],
        out_specs=(ANY, VM, VM),
        scratch_shapes=[
            pltpu.VMEM((nb, slots, bs, bs), bf16),
            pltpu.VMEM((nb, bs, width), f32),
            *tables,
            pltpu.VMEM((n, mb, bs), i32),
            pltpu.VMEM((n, mb, bs), i32),
            pltpu.VMEM((nb, bs, width), f32),
            pltpu.VMEM((nb, bs, width), f32),
            pltpu.VMEM((nb, bs, width), f32),
            pltpu.VMEM((extra + 1, bs, width), f32),
            pltpu.SMEM((extra,), i32), pltpu.SMEM((nb,), i32),
            dma, dma, dma, dma, *[dma((n,))] * (2 * trips + 2),
        ],
        compiler_params=pltpu.CompilerParams(
            collective_id=1, has_side_effects=True, vmem_limit_bytes=54 * MIB),
        name="relax",
    )(guess3, rhs3, deg2, agg2, columns.T, block_counts, send_lists[0].T, weights)

    ways = 4
    top = nc // 2
    keep, give = pl.pallas_call(
        functools.partial(restrict_kernel, ways),
        out_shape=(pltpu.VMEM((top, width), f32), pltpu.VMEM((top, width), bf16)),
        in_specs=[SM, VM],
        out_specs=(VM, VM),
        scratch_shapes=[pltpu.VMEM((nc, width), f32)] * ways,
        compiler_params=pltpu.CompilerParams(vmem_limit_bytes=36 * MIB),
        name="restrict",
    )(aggregates, vmem(res.reshape(nb * bs, width)))

    plan = stage_plan(nr, nz)
    stages = [order for order, _ in plan]
    unit = 16 * (n // 2)
    units = top // unit
    whole = sum(weight for _, weight in plan)
    marks = [units * sum(weight for _, weight in plan[:p]) // whole for p in range(len(plan) + 1)]
    parts = [(hi - lo) * unit for lo, hi in zip(marks, marks[1:])]
    stages = [order for order, part in zip(stages, parts) if part]
    parts = [part for part in parts if part]
    hops, moved = 0, 0
    for order, left in zip(stages, parts):
        for s, bits in enumerate(order):
            group = 1 << len(bits)
            hops += group - 1
            if s:
                left //= group
                moved += (group - 1) * left
    out = pl.pallas_call(
        functools.partial(cycle_kernel, parts, stages),
        out_shape=pltpu.VMEM((nb, bs, width), f32),
        in_specs=[VM, VM, VM, ANY, VM, VM, ANY, SM, SM, ANY],
        out_specs=VM,
        scratch_shapes=[
            pltpu.VMEM((nb, slots, bs, bs), bf16),
            pltpu.VMEM((top, width), bf16),
            pltpu.VMEM((moved, width), bf16),
            pltpu.VMEM((moved, width), bf16),
            pltpu.VMEM((nc, width), bf16),
            pltpu.VMEM((nc, width), f32),
            pltpu.VMEM((nt, bs, width), bf16),
            pltpu.VMEM((extra + 1, bs, width), f32),
            pltpu.VMEM((nb, bs, width), f32),
            pltpu.VMEM((nb, bs, width), f32),
            pltpu.VMEM((top // (n // 2), width), f32),
            pltpu.VMEM((bs, width), f32),
            pltpu.SMEM((nt * bs,), i32), pltpu.SMEM((extra,), i32), pltpu.SMEM((nb,), i32),
            dma((hops,)), dma((hops,)), dma((hops,)), dma((hops,)), dma((3,)),
        ],
        compiler_params=pltpu.CompilerParams(
            collective_id=2, has_side_effects=True, vmem_limit_bytes=52 * MIB if nt > 128 else 46 * MIB),
        name="cycle",
    )(vmem(give), vmem(keep), coarse_diag.reshape(nc // bs, bs), x1, vmem(res), deg2, ids.reshape(-1), columns.T, block_counts, weights)
    return out.reshape(nb * bs, width)


def solution(mesh):
    both = ("rows", "cores")
    return jax.shard_map(
        functools.partial(body, mesh.shape["rows"], mesh.shape["cores"]),
        mesh=mesh,
        in_specs=(
            P(both, None), P(both, None), P(both), P(both, None, None, None), P(both, None),
            P(both), P(both, None, None), P(both), P(),
        ),
        out_specs=P(both, None),
        check_vma=False,
    )
```

```python
import functools
import jax
import jax.numpy as jnp
from jax import lax
from jax.experimental import pallas as pl
from jax.experimental.pallas import tpu as pltpu
from jax.sharding import PartitionSpec as P

damping = 0.7
MIB = 1024 * 1024
LIMIT = 64 * 1024 * 1024 - 65536
MESH = pl.DeviceIdType.MESH
VM = pl.BlockSpec(memory_space=pltpu.VMEM)
SM = pl.BlockSpec(memory_space=pltpu.SMEM)
ANY = pl.BlockSpec(memory_space=pl.ANY)
f32, bf16, i32 = jnp.float32, jnp.bfloat16, jnp.int32


def column_of(deg, b):
    row = deg[pl.ds(b, 1), :]
    return jnp.transpose(jnp.broadcast_to(row, (row.shape[1], row.shape[1])))


def row_product(w, tab, cols, b, first, count):
    left = jnp.concatenate([w[b, first + s] for s in range(count)], axis=1)
    right = jnp.concatenate([tab[cols[first + s, b]] for s in range(count)], axis=0)
    return jnp.dot(left, right, preferred_element_type=f32)


def find_full_rows(counts, half, pick, spot):
    nb, extra = spot.shape[0], pick.shape[0]

    def look(b, found):
        rank, rows = found[0], found[1:]
        full = jnp.where(counts[b] > half, 1, 0)
        spot[b] = jnp.where(full == 1, rank, extra)
        rows = [row + jnp.where(rank == e, full * b, 0) for e, row in enumerate(rows)]
        return (rank + full, *rows)

    zero = jnp.zeros((), i32)
    found = lax.fori_loop(0, nb, look, (zero,) * (extra + 1))
    for e in range(extra):
        pick[e] = found[1 + e]


def full_products(w, tab, cols, half, pick, ex):
    for e in range(pick.shape[0]):
        ex[e] = row_product(w, tab, cols, pick[e], half, half)


def vmem(x):
    return pltpu.with_memory_space_constraint(x, pltpu.VMEM)


def each_row(count, step, act):
    @pl.loop(0, count // step)
    def _(i):
        for u in range(step):
            act(i * step + u)


def relax_kernel(nr, nz, guess_hbm, rhs_hbm, deg, agg, cols, counts, sends, w_hbm,
                 x1_out, res, ids_out,
                 w, guess, tab1, tab2, pack, aggpack, hagg, dcol, rhs, x1, ex, pick, spot,
                 wsem, bsem, gsem, xsem, s1, r1, s2, r2, sa, ra):
    n = nr * nz
    nb, half = w.shape[0], w.shape[1] // 2
    mb = pack.shape[0] // n
    me = lax.axis_index("rows") * nz + lax.axis_index("cores")
    barrier = pltpu.get_barrier_semaphore()

    def where(t):
        return (t // nz, lax.rem(t, nz))

    @pl.loop(1, n)
    def _(k):
        pl.semaphore_signal(barrier, 1, device_id=where(lax.rem(me + k, n)), device_id_type=MESH)

    weights_copy = pltpu.make_async_copy(w_hbm, w, wsem)
    rhs_copy = pltpu.make_async_copy(rhs_hbm, rhs, bsem)
    guess_copy = pltpu.make_async_copy(guess_hbm, guess, gsem)
    guess_copy.start()
    guess_copy.wait()
    weights_copy.start()
    rhs_copy.start()

    @pl.loop(0, n)
    def _(t):
        for j in range(mb):
            b = sends[j, t]
            pack[t * mb + j] = guess[b].astype(bf16)
            aggpack[t, pl.ds(j, 1), :] = agg[pl.ds(b, 1), :]

    pl.semaphore_wait(barrier, n - 1)

    def data_copy(k, tab, ss, rr):
        t = lax.rem(me + k, n)
        return pltpu.make_async_remote_copy(
            src_ref=pack.at[pl.ds(t * mb, mb)], dst_ref=tab.at[pl.ds(nb + me * mb, mb)],
            send_sem=ss.at[k], recv_sem=rr.at[k], device_id=where(t), device_id_type=MESH)

    def agg_copy(k):
        t = lax.rem(me + k, n)
        return pltpu.make_async_remote_copy(
            src_ref=aggpack.at[t], dst_ref=hagg.at[me],
            send_sem=sa.at[k], recv_sem=ra.at[k], device_id=where(t), device_id_type=MESH)

    @pl.loop(1, n)
    def _(k):
        data_copy(k, tab1, s1, r1).start()

    @pl.loop(1, n)
    def _(k):
        agg_copy(k).start()

    hagg[me] = aggpack[me]
    for j in range(mb):
        tab1[nb + me * mb + j] = pack[me * mb + j]

    @pl.loop(0, nb)
    def _(b):
        tab1[b] = guess[b].astype(bf16)
        dcol[b] = column_of(deg, b)

    find_full_rows(counts, half, pick, spot)
    ex[pick.shape[0]] = jnp.zeros(ex.shape[1:], f32)
    weights_copy.wait()
    rhs_copy.wait()

    @pl.loop(1, n)
    def _(k):
        data_copy(k, tab1, s1, r1).wait_recv()

    def sweep(b):
        d, g = dcol[b], guess[b]
        off = row_product(w, tab1, cols, b, 0, half) + ex[spot[b]]
        first = g + damping * (rhs[b] - (d * g - off)) / d
        x1[b] = first
        tab2[b] = first.astype(bf16)

    full_products(w, tab1, cols, half, pick, ex)
    each_row(nb, 8, sweep)
    x1_copy = pltpu.make_async_copy(x1, x1_out, xsem)
    x1_copy.start()

    @pl.loop(1, n)
    def _(k):
        data_copy(k, tab1, s1, r1).wait_send()
        agg_copy(k).wait()

    @pl.loop(0, n)
    def _(t):
        for j in range(mb):
            pack[t * mb + j] = x1[sends[j, t]].astype(bf16)

    @pl.loop(1, n)
    def _(k):
        data_copy(k, tab2, s2, r2).start()

    for j in range(mb):
        tab2[nb + me * mb + j] = pack[me * mb + j]
    ids_out[pl.ds(0, nb), :] = agg[...]

    @pl.loop(0, n)
    def _(t):
        ids_out[pl.ds(nb + t * mb, mb), :] = hagg[t]


    @pl.loop(1, n)
    def _(k):
        data_copy(k, tab2, s2, r2).wait_recv()

    def residue(b):
        off = row_product(w, tab2, cols, b, 0, half) + ex[spot[b]]
        res[b] = rhs[b] - (dcol[b] * x1[b] - off)

    full_products(w, tab2, cols, half, pick, ex)
    each_row(nb, 8, residue)

    @pl.loop(1, n)
    def _(k):
        data_copy(k, tab2, s2, r2).wait_send()

    x1_copy.wait()


def split_kernel(nr, nz, guess_hbm, rhs_hbm, deg, agg, cols, counts, sends, w_hbm,
                 x1_out, res, ids_out,
                 w, guess, tab1a, tab1b, tab2a, tab2b, pack1a, pack1b, pack2a, pack2b,
                 aggpack, hagg, dcol, rhs, x1, ex, pick, spot,
                 wsem, bsem, gsem, xsem, s1a, r1a, s1b, r1b, s2a, r2a, s2b, r2b, sa, ra):
    n = nr * nz
    nb, half = w.shape[0], w.shape[1] // 2
    middle = guess.shape[2] // 2
    me = lax.axis_index("rows") * nz + lax.axis_index("cores")
    barrier = pltpu.get_barrier_semaphore()
    left = lax.broadcasted_iota(i32, guess.shape[1:], 1) < middle
    trips = (
        (tab1a, pack1a, s1a, r1a), (tab1b, pack1b, s1b, r1b),
        (tab2a, pack2a, s2a, r2a), (tab2b, pack2b, s2b, r2b),
    )

    def where(t):
        return (t // nz, lax.rem(t, nz))

    def swap(block):
        return pltpu.roll(block, middle, 1)

    @pl.loop(1, n)
    def _(k):
        pl.semaphore_signal(barrier, 1, device_id=where(lax.rem(me + k, n)), device_id_type=MESH)

    weights_copy = pltpu.make_async_copy(w_hbm, w, wsem)
    rhs_copy = pltpu.make_async_copy(rhs_hbm, rhs, bsem)
    guess_copy = pltpu.make_async_copy(guess_hbm, guess, gsem)
    guess_copy.start()

    def packed(field, side, t):
        one, two = field[sends[0, t]], field[sends[1, t]]
        return (jnp.where(left, one, swap(two)) if side == 0 else jnp.where(left, swap(one), two)).astype(bf16)

    def data_copy(trip, k):
        tab, pack, ss, rr = trips[trip]
        t = lax.rem(me + k, n)
        return pltpu.make_async_remote_copy(
            src_ref=pack.at[t], dst_ref=tab.at[nb + me * 2 + trip % 2],
            send_sem=ss.at[k], recv_sem=rr.at[k], device_id=where(t), device_id_type=MESH)

    def send_all(trip):
        @pl.loop(1, n)
        def _(k):
            data_copy(trip, k).start()

    def take_all(trip):
        tab, side = trips[trip][0], trip % 2
        tab[nb + me * 2 + side] = trips[trip][1][me]

        @pl.loop(1, n)
        def _(k):
            data_copy(trip, k).wait_recv()

        @pl.loop(0, n)
        def _(t):
            tab[nb + t * 2 + 1 - side] = swap(tab[nb + t * 2 + side].astype(f32)).astype(bf16)

    def agg_copy(k):
        t = lax.rem(me + k, n)
        return pltpu.make_async_remote_copy(
            src_ref=aggpack.at[t], dst_ref=hagg.at[me],
            send_sem=sa.at[k], recv_sem=ra.at[k], device_id=where(t), device_id_type=MESH)

    guess_copy.wait()

    @pl.loop(0, n)
    def _(t):
        pack1a[t] = packed(guess, 0, t)

    pl.semaphore_wait(barrier, n - 1)
    send_all(0)
    weights_copy.start()
    rhs_copy.start()

    @pl.loop(0, n)
    def _(t):
        pack1b[t] = packed(guess, 1, t)
        for j in range(2):
            aggpack[t, pl.ds(j, 1), :] = agg[pl.ds(sends[j, t], 1), :]

    send_all(1)

    @pl.loop(1, n)
    def _(k):
        agg_copy(k).start()

    hagg[me] = aggpack[me]

    @pl.loop(0, nb)
    def _(b):
        block = guess[b].astype(bf16)
        tab1a[b] = block
        tab1b[b] = block
        dcol[b] = column_of(deg, b)

    find_full_rows(counts, half, pick, spot)
    ex[pick.shape[0]] = jnp.zeros(ex.shape[1:], f32)
    weights_copy.wait()
    rhs_copy.wait()

    def sweep(side):
        tab = trips[side][0]

        def act(b):
            d, g = dcol[b], guess[b]
            off = row_product(w, tab, cols, b, 0, half) + ex[spot[b]]
            fresh = g + damping * (rhs[b] - (d * g - off)) / d
            if side:
                fresh = jnp.where(left, x1[b], fresh)
            x1[b] = fresh
            trips[2 + side][0][b] = fresh.astype(bf16)

        take_all(side)
        full_products(w, tab, cols, half, pick, ex)
        each_row(nb, 8, act)
        pack = trips[2 + side][1]

        @pl.loop(0, n)
        def _(t):
            pack[t] = packed(x1, side, t)

        send_all(2 + side)

    sweep(0)
    sweep(1)
    x1_copy = pltpu.make_async_copy(x1, x1_out, xsem)
    x1_copy.start()

    @pl.loop(1, n)
    def _(k):
        agg_copy(k).wait()

    ids_out[pl.ds(0, nb), :] = agg[...]

    @pl.loop(0, n)
    def _(t):
        ids_out[pl.ds(nb + t * 2, 2), :] = hagg[t]

    def residue(side):
        tab = trips[2 + side][0]

        def act(b):
            off = row_product(w, tab, cols, b, 0, half) + ex[spot[b]]
            fresh = rhs[b] - (dcol[b] * x1[b] - off)
            res[b] = jnp.where(left, res[b], fresh) if side else fresh

        take_all(2 + side)
        full_products(w, tab, cols, half, pick, ex)
        each_row(nb, 8, act)

    residue(0)
    residue(1)
    for trip in range(4):
        @pl.loop(1, n)
        def _(k):
            data_copy(trip, k).wait_send()

    x1_copy.wait()


def restrict_kernel(ways, agg, res, keep, give, *accs):
    for acc in accs:
        acc[...] = jnp.zeros_like(acc)
    span = res.shape[0] // ways
    step = 8

    @pl.loop(0, span // step)
    def _(i):
        for u in range(step):
            places = [agg[q * span + i * step + u] for q in range(ways)]
            sums = [
                accs[q][pl.ds(places[q], 1), :] + res[pl.ds(q * span + i * step + u, 1), :]
                for q in range(ways)
            ]
            for q in range(ways):
                accs[q][pl.ds(places[q], 1), :] = sums[q]

    top = keep.shape[0]
    bit = lax.rem(lax.axis_index("rows"), 2)
    tile = 64

    def total(start):
        rows = pl.ds(pl.multiple_of(start, 16), tile)
        value = accs[0][rows, :]
        for acc in accs[1:]:
            value = value + acc[rows, :]
        return value

    @pl.loop(0, top // tile)
    def _(i):
        rows = pl.ds(i * tile, tile)
        give[rows, :] = total((1 - bit) * top + i * tile).astype(bf16)
        keep[rows, :] = total(bit * top + i * tile)


def cycle_kernel(parts, stages, give, keep, diag, x1_hbm, res, deg, ids_hbm, cols, counts, w_hbm, out,
                 w, first, sbuf, rbuf, corr, fine, tab, ex, base, dcol, dinv, turned, pick, spot,
                 ss, rs, sg, rg, more, *windows):
    top = keep.shape[0]
    acc = fine
    nb, half, size = w.shape[0], w.shape[1] // 2, w.shape[2]
    r, z = lax.axis_index("rows"), lax.axis_index("cores")
    barrier = pltpu.get_barrier_semaphore()
    count = len(parts)
    begin = [sum(parts[:p]) for p in range(count)]

    def mine(bit):
        axis, m = bit
        return lax.rem((r if axis == 0 else z) // m, 2)

    def peer(bits, d):
        at, index = [r, z], 0
        for i, bit in enumerate(bits):
            flip = (d >> (len(bits) - 1 - i)) & 1
            b = mine(bit)
            if flip:
                at[bit[0]] = at[bit[0]] + (1 - 2 * b) * bit[1]
                b = 1 - b
            index = index * 2 + b
        return tuple(at), index

    def rows_of(start, tile, i):
        return pl.ds(pl.multiple_of(start + i * tile, 16), tile)

    def tiled(rows, act):
        tile = 64
        while rows % tile:
            tile //= 2

        @pl.loop(0, rows // tile)
        def _(i):
            act(tile, i)

    met = []
    for order in stages:
        for bits in order:
            for d in range(1, 1 << len(bits)):
                key = tuple(sorted(bit for i, bit in enumerate(bits) if (d >> (len(bits) - 1 - i)) & 1))
                if key not in met:
                    met.append(key)
                    pl.semaphore_signal(barrier, 1, device_id=peer(bits, d)[0], device_id_type=MESH)
    others = [pltpu.make_async_copy(a, b, more.at[k]) for k, (a, b) in enumerate(((x1_hbm, base), (w_hbm, w)))]
    others[0].start()
    span = windows[0].shape[0]

    def fetch(i, k):
        part = pl.ds((i * len(windows) + k) * span, span)
        return pltpu.make_async_copy(ids_hbm.at[part], windows[k], more.at[2 + k])

    for k in range(len(windows)):
        fetch(0, k).start()
    pl.semaphore_wait(barrier, len(met))

    room, slots, at, taken = {}, {}, 0, 0
    for p in range(count):
        left = parts[p]
        for s, bits in enumerate(stages[p]):
            group = 1 << len(bits)
            if s:
                left //= group
            for d in range(1, group):
                slots[p, s, d] = taken
                taken += 1
                if s:
                    room[p, s, d] = (at, left)
                    at += left

    def hop(p, s, d):
        k = slots[p, s, d]
        if s == 0:
            rows = pl.ds(begin[p], parts[p])
            source, target = give.at[rows], first.at[rows]
        else:
            at, left = room[p, s, d]
            rows = pl.ds(at, left)
            source, target = sbuf.at[rows], rbuf.at[rows]
        return pltpu.make_async_remote_copy(
            src_ref=source, dst_ref=target, send_sem=ss.at[k], recv_sem=rs.at[k],
            device_id=peer(stages[p][s], d)[0], device_id_type=MESH)

    for p in range(count):
        hop(p, 0, 1).start()

    find_full_rows(counts, half, pick, spot)
    ex[pick.shape[0]] = jnp.zeros(ex.shape[1:], f32)
    shift = mine(stages[0][0][0]) * top

    def place_of(p):
        place, left = begin[p], parts[p]
        for bits in stages[p][1:]:
            left //= 1 << len(bits)
            place = place + peer(bits, 0)[1] * left
        return place, left

    final = 0
    spots = []
    for p in range(count):
        place, left = place_of(p)
        spots.append(final)

        @pl.loop(0, left // 16)
        def _(i):
            start = shift + place + i * 16
            turned[...] = column_of(diag, start // 128)
            dinv[pl.ds(spots[p] + i * 16, 16), :] = 1.0 / turned[pl.ds(pl.multiple_of(lax.rem(start, 128), 16), 16), :]

        final += left

    def gathered(p, s, start, rows):
        def add(tile, i):
            here = rows_of(start, tile, i)
            if s == 0:
                acc[here, :] = keep[here, :] + first[here, :].astype(f32)
            else:
                total = acc[here, :]
                for d in range(1, 1 << len(stages[p][s])):
                    total = total + rbuf[rows_of(room[p, s, d][0], tile, i), :].astype(f32)
                acc[here, :] = total

        tiled(rows, add)

    regions = list(begin)
    sizes = list(parts)
    levels = max(len(order) for order in stages)
    for s in range(1, levels):
        for p in range(count):
            if s >= len(stages[p]):
                continue
            for d in range(1, 1 << len(stages[p][s - 1])):
                hop(p, s - 1, d).wait_recv()
            gathered(p, s - 1, regions[p], sizes[p])
            bits = stages[p][s]
            left = sizes[p] >> len(bits)
            for d in range(1, 1 << len(bits)):
                start = regions[p] + peer(bits, d)[1] * left
                at = room[p, s, d][0]

                def send(tile, i):
                    sbuf[rows_of(at, tile, i), :] = acc[rows_of(start, tile, i), :].astype(bf16)

                tiled(left, send)
                hop(p, s, d).start()
            regions[p], sizes[p] = regions[p] + peer(bits, 0)[1] * left, left
        if s == 1:
            others[1].start()

            @pl.loop(0, nb)
            def _(b):
                dcol[b] = damping / column_of(deg, b)

            others[0].wait()

            @pl.loop(0, nb)
            def _(b):
                base[b] = base[b] + dcol[b] * res[b]

    def spread(p, s, d, start, left):
        rows = pl.ds(pl.multiple_of(start, 16), left)
        k = slots[p, s, d]
        return pltpu.make_async_remote_copy(
            src_ref=corr.at[rows], dst_ref=corr.at[rows], send_sem=sg.at[k], recv_sem=rg.at[k],
            device_id=peer(stages[p][s], d)[0], device_id_type=MESH)

    def widen(start, rows):
        def act(tile, i):
            fine[rows_of(start, tile, i), :] = corr[rows_of(start, tile, i), :].astype(f32)
        tiled(rows, act)

    sent, waits = [], {}
    for s in reversed(range(levels)):
        for p in range(count):
            last = len(stages[p]) - 1
            if s > last:
                continue
            if s == last:
                for d in range(1, 1 << len(stages[p][s])):
                    hop(p, s, d).wait_recv()
                start, left = regions[p], sizes[p]
                gathered(p, s, start, left)

                def settle(tile, i):
                    corr[rows_of(shift + start, tile, i), :] = (
                        acc[rows_of(start, tile, i), :] * dinv[rows_of(spots[p], tile, i), :]).astype(bf16)

                tiled(left, settle)
            else:
                for copy in waits[p]:
                    copy.wait_recv()
                bits = stages[p][s + 1]
                regions[p] = regions[p] - peer(bits, 0)[1] * sizes[p]
                sizes[p] = sizes[p] << len(bits)
            waits[p] = [
                spread(p, s, d, shift + regions[p], sizes[p]) for d in range(1, 1 << len(stages[p][s]))
            ]
            for copy in waits[p]:
                copy.start()
            sent += waits[p]
            if s == 0:
                widen(shift + begin[p], parts[p])
    for p in range(count):
        for copy in waits[p]:
            copy.wait_recv()
        widen(top - shift + begin[p], parts[p])

    step = 16

    blocks = span // size
    rounds = tab.shape[0] // (blocks * len(windows))

    @pl.loop(0, rounds)
    def _(i):
        for k, window in enumerate(windows):
            fetch(i, k).wait()
            for q in range(blocks):
                b = (i * len(windows) + k) * blocks + q
                for at in range(0, size, step):
                    tab[b, at:at + step, :] = jnp.concatenate(
                        [fine[pl.ds(window[q * size + at + u], 1), :] for u in range(step)], axis=0).astype(bf16)

            @pl.when(i + 1 < rounds)
            def _():
                fetch(i + 1, k).start()

    others[1].wait()
    full_products(w, tab, cols, half, pick, ex)

    def finish(b):
        off = row_product(w, tab, cols, b, 0, half) + ex[spot[b]]
        out[b] = base[b] + (1.0 - damping) * tab[b].astype(f32) + dcol[b] * off

    each_row(nb, 8, finish)
    for copy in sent:
        copy.wait_send()
    for p, s, d in slots:
        hop(p, s, d).wait_send()


def stage_plan(nr, nz):
    row_bits = [((0, 1 << k),) for k in range(1, nr.bit_length() - 1)]
    z_bits = [(1, 1 << k) for k in range(nz.bit_length() - 1)]
    core = [((0, 1),)]
    swapped = row_bits[::-1]
    apart, together = [(bit,) for bit in z_bits], [tuple(z_bits)]
    a = core + row_bits + together
    b = core + swapped + together
    c = core + apart + row_bits
    d = core + apart + swapped
    return 4 * [(a, 3), (b, 3), (c, 1), (d, 1)]


def body(nr, nz, rhs, guess, degree, weights, columns, block_counts, send_lists, aggregates, coarse_diag):
    n = nr * nz
    nb, slots, bs = weights.shape[0], weights.shape[1], weights.shape[2]
    width = rhs.shape[1]
    nc = coarse_diag.shape[0]
    mb = send_lists.shape[2]
    nt = nb + n * mb
    extra = nb // 4
    dma = pltpu.SemaphoreType.DMA
    rhs3, guess3 = rhs.reshape(nb, bs, width), guess.reshape(nb, bs, width)
    deg2, agg2 = degree.reshape(nb, bs), aggregates.reshape(nb, bs)
    field = jax.ShapeDtypeStruct((nb, bs, width), f32)

    table, message = pltpu.VMEM((nt, bs, width), bf16), pltpu.VMEM((n, bs, width), bf16)
    split = mb == 2 and nt <= 4 * nb
    if split:
        kernel, tables, trips = split_kernel, [table] * 4 + [message] * 4, 4
    else:
        kernel, tables, trips = relax_kernel, [table] * 2 + [pltpu.VMEM((n * mb, bs, width), bf16)], 2
    x1, res, ids = pl.pallas_call(
        functools.partial(kernel, nr, nz),
        out_shape=(field, pltpu.VMEM((nb, bs, width), f32), jax.ShapeDtypeStruct((nt, bs), i32)),
        in_specs=[ANY, ANY, VM, VM, SM, SM, SM, ANY],
        out_specs=(ANY, VM, VM),
        scratch_shapes=[
            pltpu.VMEM((nb, slots, bs, bs), bf16),
            pltpu.VMEM((nb, bs, width), f32),
            *tables,
            pltpu.VMEM((n, mb, bs), i32),
            pltpu.VMEM((n, mb, bs), i32),
            pltpu.VMEM((nb, bs, width), f32),
            pltpu.VMEM((nb, bs, width), f32),
            pltpu.VMEM((nb, bs, width), f32),
            pltpu.VMEM((extra + 1, bs, width), f32),
            pltpu.SMEM((extra,), i32), pltpu.SMEM((nb,), i32),
            dma, dma, dma, dma, *[dma((n,))] * (2 * trips + 2),
        ],
        compiler_params=pltpu.CompilerParams(
            collective_id=1, has_side_effects=True, vmem_limit_bytes=54 * MIB),
        name="relax",
    )(guess3, rhs3, deg2, agg2, columns.T, block_counts, send_lists[0].T, weights)

    ways = 4
    top = nc // 2
    keep, give = pl.pallas_call(
        functools.partial(restrict_kernel, ways),
        out_shape=(pltpu.VMEM((top, width), f32), pltpu.VMEM((top, width), bf16)),
        in_specs=[SM, VM],
        out_specs=(VM, VM),
        scratch_shapes=[pltpu.VMEM((nc, width), f32)] * ways,
        compiler_params=pltpu.CompilerParams(vmem_limit_bytes=36 * MIB),
        name="restrict",
    )(aggregates, vmem(res.reshape(nb * bs, width)))

    plan = stage_plan(nr, nz)
    stages = [order for order, _ in plan]
    unit = 16 * (n // 2)
    units = top // unit
    whole = sum(weight for _, weight in plan)
    marks = [units * sum(weight for _, weight in plan[:p]) // whole for p in range(len(plan) + 1)]
    parts = [(hi - lo) * unit for lo, hi in zip(marks, marks[1:])]
    stages = [order for order, part in zip(stages, parts) if part]
    parts = [part for part in parts if part]
    hops, moved = 0, 0
    for order, left in zip(stages, parts):
        for s, bits in enumerate(order):
            group = 1 << len(bits)
            hops += group - 1
            if s:
                left //= group
                moved += (group - 1) * left
    out = pl.pallas_call(
        functools.partial(cycle_kernel, parts, stages),
        out_shape=pltpu.VMEM((nb, bs, width), f32),
        in_specs=[VM, VM, VM, ANY, VM, VM, ANY, SM, SM, ANY],
        out_specs=VM,
        scratch_shapes=[
            pltpu.VMEM((nb, slots, bs, bs), bf16),
            pltpu.VMEM((top, width), bf16),
            pltpu.VMEM((moved, width), bf16),
            pltpu.VMEM((moved, width), bf16),
            pltpu.VMEM((nc, width), bf16),
            pltpu.VMEM((nc, width), f32),
            pltpu.VMEM((nt, bs, width), bf16),
            pltpu.VMEM((extra + 1, bs, width), f32),
            pltpu.VMEM((nb, bs, width), f32),
            pltpu.VMEM((nb, bs, width), f32),
            pltpu.VMEM((top // (n // 2), width), f32),
            pltpu.VMEM((bs, width), f32),
            pltpu.SMEM((extra,), i32), pltpu.SMEM((nb,), i32),
            dma((hops,)), dma((hops,)), dma((hops,)), dma((hops,)), dma((10,)),
            *[pltpu.SMEM((2 * bs,), i32)] * 8,
        ],
        compiler_params=pltpu.CompilerParams(
            collective_id=2, has_side_effects=True, vmem_limit_bytes=52 * MIB if nt > 128 else 46 * MIB),
        name="cycle",
    )(vmem(give), vmem(keep), coarse_diag.reshape(nc // bs, bs), x1, vmem(res), deg2, ids.reshape(-1), columns.T, block_counts, weights)
    return out.reshape(nb * bs, width)


def solution(mesh):
    both = ("rows", "cores")
    return jax.shard_map(
        functools.partial(body, mesh.shape["rows"], mesh.shape["cores"]),
        mesh=mesh,
        in_specs=(
            P(both, None), P(both, None), P(both), P(both, None, None, None), P(both, None),
            P(both), P(both, None, None), P(both), P(),
        ),
        out_specs=P(both, None),
        check_vma=False,
    )
```
